32 devices in a mesh: rep: 4 (over y, x), ep: 8 (over z, core).
Axes of the slice: x: 2, y: 2, z: 4, core: 2. Of those that a mesh axis runs over, the one named last changes fastest.
Arguments:
- out_grad: bfloat16 [2048, 2048], P(('rep', 'ep')), may hold values from -3 to 3
- saved_hidden: bfloat16 [2048, 2, 7168], P(('rep', 'ep')), may hold values from -0.59765625 to 0.59765625
- combine: bfloat16 [2048, 2], P(('rep', 'ep')), may hold values from 0.049804688 to 1
- expert_ids: int32 [2048, 2], P(('rep', 'ep')), may hold values from 0 to 7, all different within a row; in each aligned block of 64 rows (0 to 63, 64 to 127, ...) at most 24 rows name the same one
Outputs:
- down_grad: float32 [57344, 2048], P('ep', 'rep')
The draws below stay inside these ranges and needn't reach their ends.
Inputs may be any that keep to these rules, and one draw needn't show every extreme that they name: `expert_ids`: in each aligned block of 64 rows (the rows of one device), no expert is named by more than 24 slots, a bound that some block reaches; the 2 ids of a row differ; every expert is named somewhere.
All inputs are finite; a program needn't handle non-finite values.
Results may differ from the reference program's by a relative error of at most 0.0042.
Values may be sent and summed in bfloat16 or wider, within the bound.
A program may use at most 64 MiB of HBM per device.

```python
import math
import jax
import jax.numpy as jnp
import numpy as np
from jax import lax

D = 2048
FF = 7168
EXPERTS = 8
TOP = 2
TOK_DEV = 64
CAP = 24
TOKENS = 2048
N_REP = 4
N_EP = 8


def shard_levels(rng, extent, pieces, smallest, top_value):
    gain = 1.0
    for axis_at, shards_of in pieces:
        draws = jax.random.uniform(jax.random.fold_in(jax.random.fold_in(rng, 6), axis_at), (shards_of,), jnp.float32, smallest / len(pieces), top_value / len(pieces))
        gain = gain * jnp.repeat(jnp.exp(draws), extent[axis_at] // shards_of).reshape((-1,) + (1,) * (len(extent) - 1 - axis_at))
    return gain


def assign_block(rng, own, number, rows, number_of, top, limit, skew):
    order = jax.random.permutation(rng, number_of)
    packed, common = shares(number_of, rows * top, limit, skew, True), shares(number_of, rows * top, limit, skew, False)
    places = jnp.arange(number_of)

    def named(sizes, turn):
        used = int((sizes > 0).sum())
        fixed = max(1, used // 4)
        moved = fixed + (places - fixed + turn * (used - fixed)) % max(1, number_of - fixed)
        return jnp.zeros((number_of,), jnp.int32).at[order[jnp.where(places < fixed, places, moved)]].set(jnp.asarray(sizes, jnp.int32))

    sizes = jnp.where(number % 4 == 0, named(packed, number // 4), named(common, number - number // 4 - 1))
    mixed = jax.random.permutation(jax.random.fold_in(own, 3), number_of)
    donor, receiver = mixed[0:number_of // 2 * 2:2], mixed[1:number_of // 2 * 2:2]
    slack = jnp.minimum(sizes[donor] - 1, limit - sizes[receiver]) // 2
    slack = jnp.where((donor == order[0]) | (receiver == order[0]) | (sizes[receiver] == 0), 0, jnp.maximum(slack, 0))
    moved = jax.random.randint(jax.random.fold_in(own, 4), (number_of // 2,), 0, 1 << 20) % (slack + 1)
    sizes = sizes.at[donor].add(-moved).at[receiver].add(moved)
    items = jnp.searchsorted(jnp.cumsum(sizes), jnp.arange(rows * top), side="right").astype(jnp.int32)
    listing = items.reshape(top, rows).T
    listing = listing[jax.random.permutation(jax.random.fold_in(own, 1), rows)]
    turn = jax.random.randint(jax.random.fold_in(own, 2), (rows, 1), 0, top)
    return jnp.take_along_axis(listing, (jnp.arange(top)[None, :] + turn) % top, axis=1)


def shares(amount, total, bound, slope, full):
    portions = [(1 << 20) // math.isqrt(standing ** slope) + 1 for standing in range(1, amount + 1)]
    largest = bound if full else min(bound, max(-(-total // amount), total * portions[0] // sum(portions)))
    least = 1 if total - largest >= amount - 1 else 0
    holding, surplus = [largest] + [least] * (amount - 1), total - largest - least * (amount - 1)
    while surplus > 0:
        candidates = [i for i in range(1, amount) if holding[i] < largest] or [i for i in range(1, amount) if holding[i] < bound]
        pool, remaining = sum([portions[i] for i in candidates]), surplus
        for i in candidates:
            extra = min(bound - holding[i], max(1, remaining * portions[i] // pool), surplus)
            holding[i] = holding[i] + extra
            surplus = surplus - extra
    return np.array(holding)


def normal_values(own_key, shape, spread, limit, cuts=(), kind=jnp.bfloat16):
    entries = jax.random.normal(own_key, shape, jnp.float32) * spread
    if len(cuts) > 0:
        entries = shard_levels(own_key, shape, cuts, -0.22, 0.18) * entries
    return jnp.clip(entries, min=-limit, max=limit).astype(kind)


def setup_inputs(seed: int = 0) -> dict:
    streams_of = jax.random.split(jax.random.key(seed), 5)
    out_grad = normal_values(streams_of[0], (TOKENS, D), 0.5, 3.0, ((0, 32),))
    saved_hidden = normal_values(streams_of[1], (TOKENS, TOP, FF), 0.1, 0.59765625, ((0, 32),))
    combine = jnp.clip(jnp.exp(math.log(1.0) - 2.9996462 * jax.random.uniform(streams_of[2], (TOKENS, TOP), jnp.float32) ** shard_levels(streams_of[2], (TOKENS, TOP), ((0, 32),), -0.2, 0.2)), 0.049804688, 1.0).astype(jnp.bfloat16)
    expert_ids_keys = jax.random.split(jax.random.fold_in(streams_of[3], 1), TOKENS // TOK_DEV)
    expert_ids_turns = jax.random.permutation(jax.random.fold_in(streams_of[3], 3), TOKENS // TOK_DEV)
    expert_ids = jax.vmap(lambda own, number: assign_block(jax.random.fold_in(streams_of[3], 2), own, number, TOK_DEV, EXPERTS, TOP, CAP, 2))(expert_ids_keys, expert_ids_turns).reshape((TOKENS, TOP))
    return {"out_grad": out_grad, "saved_hidden": saved_hidden, "combine": combine, "expert_ids": expert_ids}


def reference(out_grad, saved_hidden, combine, expert_ids):
    tok_count = out_grad.shape[0]
    slot_count = tok_count * TOP
    most_rows = N_REP * N_EP * CAP
    flat_ids = expert_ids.reshape(slot_count).astype(jnp.int32)
    flat_prob = combine.reshape(slot_count).astype(jnp.float32)
    flat_hidden = saved_hidden.reshape(slot_count, FF)
    order = jnp.argsort(flat_ids, stable=True).astype(jnp.int32)
    onehot = (flat_ids[:, None] == jnp.arange(EXPERTS, dtype=jnp.int32)[None, :]).astype(jnp.int32)
    counts = jnp.sum(onehot, axis=0).astype(jnp.int32)
    starts = (jnp.cumsum(counts) - counts).astype(jnp.int32)
    padded_order = jnp.concatenate([order, jnp.zeros((most_rows,), jnp.int32)])

    def one_expert(expert):
        chosen = lax.dynamic_slice_in_dim(padded_order, starts[expert], most_rows).astype(jnp.int32)
        valid = jnp.arange(most_rows, dtype=jnp.int32) < counts[expert]
        grad_rows = out_grad[chosen // TOP]
        prob = jnp.where(valid, flat_prob[chosen], jnp.float32(0.0))
        hidden = flat_hidden[chosen]
        scaled = (prob[:, None] * grad_rows.astype(jnp.float32)).astype(jnp.bfloat16)
        return lax.dot_general(hidden, scaled, (((0,), (0,)), ((), ())), preferred_element_type=jnp.float32)

    wgrad_all = lax.map(one_expert, jnp.arange(EXPERTS, dtype=jnp.int32))
    return wgrad_all.reshape(EXPERTS * FF, out_grad.shape[1])
```

```python
import functools

import jax
import jax.numpy as jnp
from jax import lax
from jax.experimental import pallas as pl
from jax.experimental.pallas import tpu as pltpu
from jax.sharding import PartitionSpec as P

EXPERTS = 8
TOP = 2
CAP = 24
MESH = pl.DeviceIdType.MESH


def xor(place, pattern):
    bit = 1
    while bit <= pattern:
        if pattern & bit:
            place = place + bit - 2 * bit * ((place // bit) % 2)
        bit *= 2
    return place


def partners(ep_count):
    pairs = ep_count // 2
    if ep_count & (ep_count - 1) == 0 and pairs >= 2:
        chips = [pairs - 1] + list(range(1, pairs - 1))
        order = [0, 1] + [2 * chip + core for chip in chips for core in (0, 1)]
        return [(lambda p, k=k: xor(p, k), lambda p, k=k: xor(p, k)) for k in order]
    return [
        (lambda p, k=k: (p + k) % ep_count, lambda p, k=k: (p + ep_count - k) % ep_count)
        for k in range(ep_count)
    ]


def ring_place(rep_count):
    if rep_count == 4:
        swap = lambda q: q + q // 2 - 2 * (q // 3)
        return swap, swap
    return (lambda q: q), (lambda q: q)


def exchange_kernel(
    rep_count, ep_count, hidden_ref, grad_ref, rows_ref, cols_ref,
    own_sem, send_sem, recv_sem, ring_send, ring_recv, grad_send, grad_recv,
):
    rep, ep = lax.axis_index("rep"), lax.axis_index("ep")
    group = ep_count // EXPERTS
    unit_cols = rows_ref.shape[3]
    col_width = cols_ref.shape[3]
    to_ring, from_ring = ring_place(rep_count)
    place = to_ring(rep)
    at = lambda off: from_ring((place + off + rep_count) % rep_count)
    steps = partners(ep_count)
    full_hops = (rep_count - 1) // 2
    half_hop = rep_count % 2 == 0
    half = unit_cols // 2 // 128 * 128
    parts = {0: pl.ds(0, half), 1: pl.ds(half, unit_cols - half)}

    def piece_for(dest):
        start = pl.multiple_of((dest % group) * unit_cols, 128)
        return hidden_ref.at[dest // group, :, pl.ds(start, unit_cols)]

    def remote(src, dst, send, recv, to_rep, to_ep):
        return pltpu.make_async_remote_copy(
            src_ref=src, dst_ref=dst, send_sem=send, recv_sem=recv,
            device_id=(to_rep, to_ep), device_id_type=MESH,
        )

    started = []
    own = pltpu.make_async_copy(piece_for(ep), rows_ref.at[rep, ep], own_sem.at[0])
    own_cols = pltpu.make_async_copy(
        grad_ref.at[ep // group, :, pl.ds(pl.multiple_of(rep * col_width, 128), col_width)],
        cols_ref.at[rep, ep], own_sem.at[1],
    )

    exchanges = [None]
    for i in range(1, ep_count):
        dest = steps[i][0](ep)
        exchanges.append(
            remote(piece_for(dest), rows_ref.at[rep, ep], send_sem.at[i], recv_sem.at[i], rep, dest)
        )

    def hop(i, way, distance):
        source = steps[i][1](ep)
        origin = at(-way * (distance - 1))
        src = rows_ref.at[origin, source]
        dst = rows_ref.at[origin, source]
        if distance == 1 and i == 0:
            src = piece_for(ep)
        if distance > full_hops:
            cut = parts[0 if way == 1 else 1]
            src, dst = src.at[:, cut], dst.at[:, cut]
        lane = (0 if way == 1 else 1, distance - 1, i)
        return remote(src, dst, ring_send.at[lane], ring_recv.at[lane], at(way), ep)

    last_hop = full_hops + (1 if half_hop else 0)
    grads = []

    def send_grads():
        for r in range(rep_count):
            for i in range(ep_count):
                if r == 0 and i == 0:
                    continue
                to_rep, to_ep = at(r), steps[i][0](ep)
                start = pl.multiple_of(to_rep * col_width, 128)
                copy = remote(
                    grad_ref.at[to_ep // group, :, pl.ds(start, col_width)],
                    cols_ref.at[rep, ep], grad_send.at[r, i], grad_recv.at[r, i], to_rep, to_ep,
                )
                copy.start()
                grads.append(copy)

    for copy in exchanges[1:2]:
        copy.start()
    hops = {}

    def start_hop(i, distance):
        if distance > last_hop:
            return
        for way in (1, -1):
            hops[i, way, distance] = hop(i, way, distance)
            hops[i, way, distance].start()

    start_hop(0, 1)
    for copy in exchanges[2:]:
        copy.start()
    own.start()
    own_cols.start()
    for i in range(1, ep_count + last_hop):
        if i < ep_count:
            exchanges[i].wait_recv()
            start_hop(i, 1)
        if i == 1:
            send_grads()
        for distance in range(1, last_hop + 1):
            j = i - distance
            if 0 <= j < ep_count:
                for way in (1, -1):
                    hops[j, way, distance].wait_recv()
                start_hop(j, distance + 1)
    for copy in grads:
        copy.wait()
    for copy in exchanges[1:]:
        copy.wait_send()
    for copy in hops.values():
        copy.wait_send()
    own.wait()
    own_cols.wait()


def exchange(hidden, grad, rep_count, ep_count):
    unit_cols = hidden.shape[2] * EXPERTS // ep_count
    col_width = grad.shape[2] // rep_count
    hops = max(1, rep_count // 2)
    return pl.pallas_call(
        functools.partial(exchange_kernel, rep_count, ep_count),
        out_shape=(
            jax.ShapeDtypeStruct((rep_count, ep_count, CAP, unit_cols), jnp.bfloat16),
            jax.ShapeDtypeStruct((rep_count, ep_count, CAP, col_width), jnp.bfloat16),
        ),
        in_specs=[pl.BlockSpec(memory_space=pl.ANY)] * 2,
        out_specs=(pl.BlockSpec(memory_space=pl.ANY),) * 2,
        scratch_shapes=[
            pltpu.SemaphoreType.DMA((2,)),
            pltpu.SemaphoreType.DMA((ep_count,)),
            pltpu.SemaphoreType.DMA((ep_count,)),
            pltpu.SemaphoreType.DMA((2, hops, ep_count)),
            pltpu.SemaphoreType.DMA((2, hops, ep_count)),
            pltpu.SemaphoreType.DMA((rep_count, ep_count)),
            pltpu.SemaphoreType.DMA((rep_count, ep_count)),
        ],
        compiler_params=pltpu.CompilerParams(has_side_effects=True),
    )(hidden, grad)


def per_device(out_grad, saved_hidden, combine, expert_ids):
    ep_count = lax.axis_size("ep")
    rep_count = lax.axis_size("rep")
    tok_count, model_width = out_grad.shape
    slot_count = tok_count * TOP
    units = saved_hidden.shape[2]
    flat_ids = expert_ids.reshape(slot_count)
    onehot = (flat_ids[:, None] == jnp.arange(EXPERTS, dtype=jnp.int32)[None, :]).astype(jnp.int32)
    slot_place = jnp.sum((jnp.cumsum(onehot, axis=0) - 1) * onehot, axis=1)
    row_of_slot = (flat_ids * CAP + slot_place).reshape(tok_count, TOP)
    packed = jnp.arange(EXPERTS * CAP, dtype=jnp.int32)
    pick = packed[:, None, None] == row_of_slot[None]
    pick_token = jnp.any(pick, axis=2).astype(jnp.bfloat16)
    packed_prob = jnp.sum(
        jnp.where(pick, combine[None].astype(jnp.float32), jnp.float32(0.0)), axis=(1, 2)
    )
    send_hidden = lax.dot_general(
        pick.astype(jnp.bfloat16).reshape(EXPERTS * CAP, slot_count),
        saved_hidden.reshape(slot_count, units),
        (((1,), (0,)), ((), ())),
        preferred_element_type=jnp.float32,
    ).astype(jnp.bfloat16)
    grad_rows = jnp.dot(pick_token, out_grad, preferred_element_type=jnp.float32)
    send_grad = (packed_prob[:, None] * grad_rows).astype(jnp.bfloat16)
    rows, cols = exchange(
        send_hidden.reshape(EXPERTS, CAP, units),
        send_grad.reshape(EXPERTS, CAP, model_width),
        rep_count,
        ep_count,
    )
    row_total = rep_count * ep_count * CAP
    return lax.dot_general(
        rows.reshape(row_total, rows.shape[3]),
        cols.reshape(row_total, cols.shape[3]),
        (((0,), (0,)), ((), ())),
        preferred_element_type=jnp.float32,
    )


def solution(mesh):
    in_specs = (
        P(("rep", "ep"), None),
        P(("rep", "ep"), None, None),
        P(("rep", "ep"), None),
        P(("rep", "ep"), None),
    )
    out_specs = P("ep", "rep")
    return jax.shard_map(
        per_device, mesh=mesh, in_specs=in_specs, out_specs=out_specs, check_vma=False
    )
```

```python
import functools

import jax
import jax.numpy as jnp
from jax import lax
from jax.experimental import pallas as pl
from jax.experimental.pallas import tpu as pltpu
from jax.sharding import PartitionSpec as P

EXPERTS = 8
TOP = 2
CAP = 24
MESH = pl.DeviceIdType.MESH


def xor(place, pattern):
    bit = 1
    while bit <= pattern:
        if pattern & bit:
            place = place + bit - 2 * bit * ((place // bit) % 2)
        bit *= 2
    return place


def partners(ep_count):
    pairs = ep_count // 2
    if ep_count & (ep_count - 1) == 0 and pairs >= 2:
        chips = [pairs - 1] + list(range(1, pairs - 1))
        order = [0, 1] + [2 * chip + core for chip in chips for core in (0, 1)]
        return [(lambda p, k=k: xor(p, k), lambda p, k=k: xor(p, k)) for k in order]
    return [
        (lambda p, k=k: (p + k) % ep_count, lambda p, k=k: (p + ep_count - k) % ep_count)
        for k in range(ep_count)
    ]


def ring_place(rep_count):
    if rep_count == 4:
        swap = lambda q: q + q // 2 - 2 * (q // 3)
        return swap, swap
    return (lambda q: q), (lambda q: q)


def exchange_kernel(
    rep_count, ep_count, hidden_ref, grad_ref, rows_ref, cols_ref,
    own_sem, send_sem, recv_sem, ring_send, ring_recv, grad_send, grad_recv,
):
    rep, ep = lax.axis_index("rep"), lax.axis_index("ep")
    group = ep_count // EXPERTS
    unit_cols = rows_ref.shape[3]
    col_width = cols_ref.shape[3]
    to_ring, from_ring = ring_place(rep_count)
    place = to_ring(rep)
    at = lambda off: from_ring((place + off + rep_count) % rep_count)
    steps = partners(ep_count)
    full_hops = (rep_count - 1) // 2
    half_hop = rep_count % 2 == 0
    half = unit_cols // 2 // 128 * 128
    parts = {0: pl.ds(0, half), 1: pl.ds(half, unit_cols - half)}

    def piece_for(dest):
        start = pl.multiple_of((dest % group) * unit_cols, 128)
        return hidden_ref.at[dest // group, :, pl.ds(start, unit_cols)]

    def remote(src, dst, send, recv, to_rep, to_ep):
        return pltpu.make_async_remote_copy(
            src_ref=src, dst_ref=dst, send_sem=send, recv_sem=recv,
            device_id=(to_rep, to_ep), device_id_type=MESH,
        )

    started = []
    own = pltpu.make_async_copy(piece_for(ep), rows_ref.at[rep, ep], own_sem.at[0])
    own_cols = pltpu.make_async_copy(
        grad_ref.at[ep // group, :, pl.ds(pl.multiple_of(rep * col_width, 128), col_width)],
        cols_ref.at[rep, ep], own_sem.at[1],
    )

    exchanges = [None]
    for i in range(1, ep_count):
        dest = steps[i][0](ep)
        exchanges.append(
            remote(piece_for(dest), rows_ref.at[rep, ep], send_sem.at[i], recv_sem.at[i], rep, dest)
        )

    def hop(i, way, distance):
        source = steps[i][1](ep)
        origin = at(-way * (distance - 1))
        src = rows_ref.at[origin, source]
        dst = rows_ref.at[origin, source]
        if distance == 1 and i == 0:
            src = piece_for(ep)
        if distance > full_hops:
            cut = parts[0 if way == 1 else 1]
            src, dst = src.at[:, cut], dst.at[:, cut]
        lane = (0 if way == 1 else 1, distance - 1, i)
        return remote(src, dst, ring_send.at[lane], ring_recv.at[lane], at(way), ep)

    last_hop = full_hops + (1 if half_hop else 0)
    grads = []

    def send_grads():
        for r in range(rep_count):
            for i in range(ep_count):
                if r == 0 and i == 0:
                    continue
                to_rep, to_ep = at(r), steps[i][0](ep)
                start = pl.multiple_of(to_rep * col_width, 128)
                copy = remote(
                    grad_ref.at[to_ep // group, :, pl.ds(start, col_width)],
                    cols_ref.at[rep, ep], grad_send.at[r, i], grad_recv.at[r, i], to_rep, to_ep,
                )
                copy.start()
                grads.append(copy)

    for copy in exchanges[1:2]:
        copy.start()
    hops = {}

    def start_hop(i, distance):
        if distance > last_hop:
            return
        for way in (1, -1):
            hops[i, way, distance] = hop(i, way, distance)
            hops[i, way, distance].start()

    start_hop(0, 1)
    for copy in exchanges[2:]:
        copy.start()
    own.start()
    own_cols.start()
    for i in range(1, ep_count + last_hop):
        if i < ep_count:
            exchanges[i].wait_recv()
            start_hop(i, 1)
        if i == 1:
            send_grads()
        for distance in range(1, last_hop + 1):
            j = i - distance
            if 0 <= j < ep_count:
                for way in (1, -1):
                    hops[j, way, distance].wait_recv()
                start_hop(j, distance + 1)
    for copy in grads:
        copy.wait()
    for copy in exchanges[1:]:
        copy.wait_send()
    for copy in hops.values():
        copy.wait_send()
    own.wait()
    own_cols.wait()


def exchange(hidden, grad, rep_count, ep_count):
    unit_cols = hidden.shape[2] * EXPERTS // ep_count
    col_width = grad.shape[2] // rep_count
    hops = max(1, rep_count // 2)
    return pl.pallas_call(
        functools.partial(exchange_kernel, rep_count, ep_count),
        out_shape=(
            jax.ShapeDtypeStruct((rep_count, ep_count, CAP, unit_cols), jnp.bfloat16),
            jax.ShapeDtypeStruct((rep_count, ep_count, CAP, col_width), jnp.bfloat16),
        ),
        in_specs=[pl.BlockSpec(memory_space=pl.ANY)] * 2,
        out_specs=(pl.BlockSpec(memory_space=pl.ANY),) * 2,
        scratch_shapes=[
            pltpu.SemaphoreType.DMA((2,)),
            pltpu.SemaphoreType.DMA((ep_count,)),
            pltpu.SemaphoreType.DMA((ep_count,)),
            pltpu.SemaphoreType.DMA((2, hops, ep_count)),
            pltpu.SemaphoreType.DMA((2, hops, ep_count)),
            pltpu.SemaphoreType.DMA((rep_count, ep_count)),
            pltpu.SemaphoreType.DMA((rep_count, ep_count)),
        ],
        compiler_params=pltpu.CompilerParams(has_side_effects=True, vmem_limit_bytes=1024 * 1024),
    )(hidden, grad)


def per_device(out_grad, saved_hidden, combine, expert_ids):
    ep_count = lax.axis_size("ep")
    rep_count = lax.axis_size("rep")
    tok_count, model_width = out_grad.shape
    slot_count = tok_count * TOP
    units = saved_hidden.shape[2]
    flat_ids = expert_ids.reshape(slot_count)
    onehot = (flat_ids[:, None] == jnp.arange(EXPERTS, dtype=jnp.int32)[None, :]).astype(jnp.int32)
    slot_place = jnp.sum((jnp.cumsum(onehot, axis=0) - 1) * onehot, axis=1)
    row_of_slot = (flat_ids * CAP + slot_place).reshape(tok_count, TOP)
    packed = jnp.arange(EXPERTS * CAP, dtype=jnp.int32)
    pick = packed[:, None, None] == row_of_slot[None]
    pick_token = jnp.any(pick, axis=2).astype(jnp.bfloat16)
    packed_prob = jnp.sum(
        jnp.where(pick, combine[None].astype(jnp.float32), jnp.float32(0.0)), axis=(1, 2)
    )
    send_hidden = lax.dot_general(
        pick.astype(jnp.bfloat16).reshape(EXPERTS * CAP, slot_count),
        saved_hidden.reshape(slot_count, units),
        (((1,), (0,)), ((), ())),
        preferred_element_type=jnp.float32,
    ).astype(jnp.bfloat16)
    grad_rows = jnp.dot(pick_token, out_grad, preferred_element_type=jnp.float32)
    send_grad = (packed_prob[:, None] * grad_rows).astype(jnp.bfloat16)
    rows, cols = exchange(
        send_hidden.reshape(EXPERTS, CAP, units),
        send_grad.reshape(EXPERTS, CAP, model_width),
        rep_count,
        ep_count,
    )
    row_total = rep_count * ep_count * CAP
    return lax.dot_general(
        rows.reshape(row_total, rows.shape[3]),
        cols.reshape(row_total, cols.shape[3]),
        (((0,), (0,)), ((), ())),
        preferred_element_type=jnp.float32,
    )


def solution(mesh):
    in_specs = (
        P(("rep", "ep"), None),
        P(("rep", "ep"), None, None),
        P(("rep", "ep"), None),
        P(("rep", "ep"), None),
    )
    out_specs = P("ep", "rep")
    return jax.shard_map(
        per_device, mesh=mesh, in_specs=in_specs, out_specs=out_specs, check_vma=False
    )
```

```python
import functools

import jax
import jax.numpy as jnp
from jax import lax
from jax.experimental import pallas as pl
from jax.experimental.pallas import tpu as pltpu
from jax.sharding import PartitionSpec as P

EXPERTS = 8
TOP = 2
CAP = 24
MESH = pl.DeviceIdType.MESH


def xor(place, pattern):
    bit = 1
    while bit <= pattern:
        if pattern & bit:
            place = place + bit - 2 * bit * ((place // bit) % 2)
        bit *= 2
    return place


def partners(ep_count):
    pairs = ep_count // 2
    if ep_count & (ep_count - 1) == 0 and pairs >= 2:
        chips = [pairs - 1] + list(range(1, pairs - 1))
        order = [0, 1] + [2 * chip + core for chip in chips for core in (0, 1)]
        return [(lambda p, k=k: xor(p, k), lambda p, k=k: xor(p, k)) for k in order]
    return [
        (lambda p, k=k: (p + k) % ep_count, lambda p, k=k: (p + ep_count - k) % ep_count)
        for k in range(ep_count)
    ]


def ring_place(rep_count):
    if rep_count == 4:
        swap = lambda q: q + q // 2 - 2 * (q // 3)
        return swap, swap
    return (lambda q: q), (lambda q: q)


def exchange_kernel(
    rep_count, ep_count, hidden_ref, grad_ref, route_ref, rows_ref, cols_ref,
    grads, routes, packed, own_sem, send_sem, recv_sem, ring_send, ring_recv,
    grad_send, grad_recv, route_send, route_recv, cols_send, cols_recv,
):
    rep, ep = lax.axis_index("rep"), lax.axis_index("ep")
    group = ep_count // EXPERTS
    unit_cols = rows_ref.shape[3]
    col_width = cols_ref.shape[3]
    to_ring, from_ring = ring_place(rep_count)
    place = to_ring(rep)
    at = lambda off: from_ring((place + off + rep_count) % rep_count)
    steps = partners(ep_count)
    full_hops = (rep_count - 1) // 2
    last_hop = rep_count // 2
    half = unit_cols // 2 // 128 * 128
    parts = {1: pl.ds(0, half), -1: pl.ds(half, unit_cols - half)}

    def piece_for(dest):
        start = pl.multiple_of((dest % group) * unit_cols, 128)
        return hidden_ref.at[dest // group, :, pl.ds(start, unit_cols)]

    def grad_cols(owner):
        return grad_ref.at[:, pl.ds(pl.multiple_of(owner * col_width, 128), col_width)]

    def remote(src, dst, send, recv, to_rep, to_ep):
        return pltpu.make_async_remote_copy(
            src_ref=src, dst_ref=dst, send_sem=send, recv_sem=recv,
            device_id=(to_rep, to_ep), device_id_type=MESH,
        )

    def hop(i, way, distance):
        source = steps[i][1](ep)
        origin = at(-way * (distance - 1))
        src = dst = rows_ref.at[origin, source]
        if distance == 1 and i == 0:
            src = piece_for(ep)
        if distance > full_hops:
            src, dst = src.at[:, parts[way]], dst.at[:, parts[way]]
        lane = (0 if way == 1 else 1, distance - 1, i)
        return remote(src, dst, ring_send.at[lane], ring_recv.at[lane], at(way), ep)

    hops = {}

    def start_hop(i, distance):
        if distance > last_hop:
            return
        for way in (1, -1):
            hops[i, way, distance] = hop(i, way, distance)
            hops[i, way, distance].start()

    near = []
    for r in range(1, rep_count):
        near.append(remote(route_ref, routes.at[rep], route_send.at[r], route_recv.at[r], at(r), ep))
        near.append(remote(grad_cols(at(r)), grads.at[rep], grad_send.at[r], grad_recv.at[r], at(r), ep))
    exchanges = [None]
    for i in range(1, ep_count):
        dest = steps[i][0](ep)
        exchanges.append(
            remote(piece_for(dest), rows_ref.at[rep, ep], send_sem.at[i], recv_sem.at[i], rep, dest)
        )
    own = [
        pltpu.make_async_copy(route_ref, routes.at[rep], own_sem.at[0]),
        pltpu.make_async_copy(grad_cols(rep), grads.at[rep], own_sem.at[1]),
        pltpu.make_async_copy(piece_for(ep), rows_ref.at[rep, ep], own_sem.at[2]),
    ]

    def pack(r):
        tok_count = grads.shape[1]
        lanes = routes.shape[2]
        route = routes[r].astype(jnp.float32)
        weight, named = route[:EXPERTS], route[EXPERTS:]
        before = (
            lax.broadcasted_iota(jnp.int32, (lanes, lanes), 0)
            < lax.broadcasted_iota(jnp.int32, (lanes, lanes), 1)
        ).astype(jnp.float32).astype(jnp.bfloat16)
        row = jnp.dot(named.astype(jnp.bfloat16), before, preferred_element_type=jnp.float32)
        row = jnp.where(named > 0.5, row, -1.0)
        slots = lax.broadcasted_iota(jnp.int32, (CAP, lanes), 0).astype(jnp.float32)
        picks = jnp.concatenate(
            [jnp.where(row[e : e + 1] == slots, weight[e : e + 1], 0.0) for e in range(EXPERTS)], axis=0
        ).astype(jnp.bfloat16)
        scaled = jnp.dot(picks[:, :tok_count], grads[r], preferred_element_type=jnp.float32)
        for e in range(EXPERTS):
            packed[r, e] = scaled[e * CAP : (e + 1) * CAP].astype(jnp.bfloat16)

    for copy in near:
        copy.start()
    exchanges[1].start()
    start_hop(0, 1)
    for copy in exchanges[2:]:
        copy.start()
    for copy in own:
        copy.start()
    spread = []
    for i in range(1, ep_count + last_hop):
        if i < ep_count:
            exchanges[i].wait_recv()
            start_hop(i, 1)
        if i == 1:
            for copy in near:
                copy.wait()
            for copy in own:
                copy.wait()
            for r in range(rep_count):
                pack(r)
        for distance in range(1, last_hop + 1):
            j = i - distance
            if 0 <= j < ep_count:
                for way in (1, -1):
                    hops[j, way, distance].wait_recv()
                start_hop(j, distance + 1)
        if i == 1:
            spread.append(
                pltpu.make_async_copy(packed.at[:, ep // group], cols_ref.at[:, ep], own_sem.at[3])
            )
            for k in range(1, ep_count):
                dest = steps[k][0](ep)
                spread.append(
                    remote(
                        packed.at[:, dest // group], cols_ref.at[:, ep],
                        cols_send.at[k], cols_recv.at[k], rep, dest,
                    )
                )
            for copy in spread:
                copy.start()
    for copy in spread:
        copy.wait()
    for copy in exchanges[1:]:
        copy.wait_send()
    for copy in hops.values():
        copy.wait_send()


def exchange(hidden, grad, route, rep_count, ep_count):
    unit_cols = hidden.shape[2] * EXPERTS // ep_count
    tok_count = grad.shape[0]
    col_width = grad.shape[1] // rep_count
    hops = max(1, rep_count // 2)
    dma = pltpu.SemaphoreType.DMA
    return pl.pallas_call(
        functools.partial(exchange_kernel, rep_count, ep_count),
        out_shape=(
            jax.ShapeDtypeStruct((rep_count, ep_count, CAP, unit_cols), jnp.bfloat16),
            jax.ShapeDtypeStruct((rep_count, ep_count, CAP, col_width), jnp.bfloat16),
        ),
        in_specs=[pl.BlockSpec(memory_space=pl.ANY)] * 3,
        out_specs=(pl.BlockSpec(memory_space=pl.ANY),) * 2,
        scratch_shapes=[
            pltpu.VMEM((rep_count, tok_count, col_width), jnp.bfloat16),
            pltpu.VMEM((rep_count,) + route.shape, jnp.bfloat16),
            pltpu.VMEM((rep_count, EXPERTS, CAP, col_width), jnp.bfloat16),
            dma((4,)),
            dma((ep_count,)),
            dma((ep_count,)),
            dma((2, hops, ep_count)),
            dma((2, hops, ep_count)),
            dma((rep_count,)),
            dma((rep_count,)),
            dma((rep_count,)),
            dma((rep_count,)),
            dma((ep_count,)),
            dma((ep_count,)),
        ],
        compiler_params=pltpu.CompilerParams(
            has_side_effects=True, vmem_limit_bytes=4 * 1024 * 1024
        ),
    )(hidden, grad, route)


def per_device(out_grad, saved_hidden, combine, expert_ids):
    ep_count = lax.axis_size("ep")
    rep_count = lax.axis_size("rep")
    tok_count, model_width = out_grad.shape
    units = saved_hidden.shape[2]
    lanes = -(-tok_count // 128) * 128
    ids, probs = expert_ids.T, combine.T
    experts = jnp.arange(EXPERTS, dtype=jnp.int32)
    chosen = ids[:, None, :] == experts[None, :, None]
    named = jnp.any(chosen, axis=0)
    weight = jnp.sum(jnp.where(chosen, probs[:, None, :].astype(jnp.float32), jnp.float32(0.0)), axis=0)
    route = jnp.concatenate([weight, named.astype(jnp.float32)], axis=0).astype(jnp.bfloat16)
    route = jnp.pad(route, ((0, 0), (0, lanes - tok_count)))
    before = jnp.arange(tok_count)[:, None] < jnp.arange(tok_count)[None, :]
    row = jnp.dot(
        named.astype(jnp.bfloat16), before.astype(jnp.bfloat16), preferred_element_type=jnp.float32
    )
    slots = jnp.arange(CAP, dtype=jnp.float32)
    at_slot = row[:, None, None, :] == slots[None, :, None, None]
    pick = (at_slot & chosen.transpose(1, 0, 2)[:, None]).astype(jnp.bfloat16)
    send_hidden = lax.dot_general(
        pick.reshape(EXPERTS * CAP, TOP, tok_count),
        saved_hidden,
        (((1, 2), (1, 0)), ((), ())),
        preferred_element_type=jnp.float32,
    ).astype(jnp.bfloat16)
    rows, cols = exchange(
        send_hidden.reshape(EXPERTS, CAP, units), out_grad, route, rep_count, ep_count
    )
    row_total = rep_count * ep_count * CAP
    return lax.dot_general(
        rows.reshape(row_total, rows.shape[3]),
        cols.reshape(row_total, cols.shape[3]),
        (((0,), (0,)), ((), ())),
        preferred_element_type=jnp.float32,
    )


def solution(mesh):
    in_specs = (
        P(("rep", "ep"), None),
        P(("rep", "ep"), None, None),
        P(("rep", "ep"), None),
        P(("rep", "ep"), None),
    )
    out_specs = P("ep", "rep")
    return jax.shard_map(
        per_device, mesh=mesh, in_specs=in_specs, out_specs=out_specs, check_vma=False
    )
```

```python
import functools

import jax
import jax.numpy as jnp
from jax import lax
from jax.experimental import pallas as pl
from jax.experimental.pallas import tpu as pltpu
from jax.sharding import PartitionSpec as P

EXPERTS = 8
TOP = 2
CAP = 24
MESH = pl.DeviceIdType.MESH


def xor(place, pattern):
    bit = 1
    while bit <= pattern:
        if pattern & bit:
            place = place + bit - 2 * bit * ((place // bit) % 2)
        bit *= 2
    return place


def partners(ep_count):
    pairs = ep_count // 2
    if ep_count & (ep_count - 1) == 0 and pairs >= 2:
        chips = [pairs - 1] + list(range(1, pairs - 1))
        order = [0, 1] + [2 * chip + core for chip in chips for core in (0, 1)]
        return [(lambda p, k=k: xor(p, k), lambda p, k=k: xor(p, k)) for k in order]
    return [
        (lambda p, k=k: (p + k) % ep_count, lambda p, k=k: (p + ep_count - k) % ep_count)
        for k in range(ep_count)
    ]


def ring_place(rep_count):
    if rep_count == 4:
        swap = lambda q: q + q // 2 - 2 * (q // 3)
        return swap, swap
    return (lambda q: q), (lambda q: q)


def exchange_kernel(
    rep_count, ep_count, hidden_ref, grad_ref, route_ref, rows_ref, cols_ref,
    grads, routes, packed, own_sem, send_sem, recv_sem, ring_send, ring_recv,
    grad_send, grad_recv, route_send, route_recv, cols_send, cols_recv,
):
    rep, ep = lax.axis_index("rep"), lax.axis_index("ep")
    group = ep_count // EXPERTS
    unit_cols = rows_ref.shape[3]
    col_width = cols_ref.shape[3]
    to_ring, from_ring = ring_place(rep_count)
    place = to_ring(rep)
    at = lambda off: from_ring((place + off + rep_count) % rep_count)
    steps = partners(ep_count)
    full_hops = (rep_count - 1) // 2
    last_hop = rep_count // 2
    half = unit_cols // 2 // 128 * 128
    parts = {1: pl.ds(0, half), -1: pl.ds(half, unit_cols - half)}

    def piece_for(dest):
        start = pl.multiple_of((dest % group) * unit_cols, 128)
        return hidden_ref.at[dest // group, :, pl.ds(start, unit_cols)]

    def grad_cols(owner):
        return grad_ref.at[:, pl.ds(pl.multiple_of(owner * col_width, 128), col_width)]

    def remote(src, dst, send, recv, to_rep, to_ep):
        return pltpu.make_async_remote_copy(
            src_ref=src, dst_ref=dst, send_sem=send, recv_sem=recv,
            device_id=(to_rep, to_ep), device_id_type=MESH,
        )

    def hop(i, way, distance):
        source = steps[i][1](ep)
        origin = at(-way * (distance - 1))
        src = dst = rows_ref.at[origin, source]
        if distance == 1 and i == 0:
            src = piece_for(ep)
        if distance > full_hops:
            src, dst = src.at[:, parts[way]], dst.at[:, parts[way]]
        lane = (0 if way == 1 else 1, distance - 1, i)
        return remote(src, dst, ring_send.at[lane], ring_recv.at[lane], at(way), ep)

    hops = {}

    def start_hop(i, distance):
        if distance > last_hop:
            return
        for way in (1, -1):
            hops[i, way, distance] = hop(i, way, distance)
            hops[i, way, distance].start()

    near = []
    for r in range(1, rep_count):
        near.append(remote(route_ref, routes.at[rep], route_send.at[r], route_recv.at[r], at(r), ep))
        near.append(remote(grad_cols(at(r)), grads.at[rep], grad_send.at[r], grad_recv.at[r], at(r), ep))
    exchanges = [None]
    for i in range(1, ep_count):
        dest = steps[i][0](ep)
        exchanges.append(
            remote(piece_for(dest), rows_ref.at[rep, ep], send_sem.at[i], recv_sem.at[i], rep, dest)
        )
    own = [
        pltpu.make_async_copy(route_ref, routes.at[rep], own_sem.at[0]),
        pltpu.make_async_copy(grad_cols(rep), grads.at[rep], own_sem.at[1]),
        pltpu.make_async_copy(piece_for(ep), rows_ref.at[rep, ep], own_sem.at[2]),
    ]

    def pack(r):
        tok_count = grads.shape[1]
        lanes = routes.shape[2]
        route = routes[r].astype(jnp.float32)
        weight, named = route[:EXPERTS], route[EXPERTS:]
        before = (
            lax.broadcasted_iota(jnp.int32, (lanes, lanes), 0)
            < lax.broadcasted_iota(jnp.int32, (lanes, lanes), 1)
        ).astype(jnp.float32).astype(jnp.bfloat16)
        row = jnp.dot(named.astype(jnp.bfloat16), before, preferred_element_type=jnp.float32)
        row = jnp.where(named > 0.5, row, -1.0)
        slots = lax.broadcasted_iota(jnp.int32, (CAP, lanes), 0).astype(jnp.float32)
        picks = jnp.concatenate(
            [jnp.where(row[e : e + 1] == slots, weight[e : e + 1], 0.0) for e in range(EXPERTS)], axis=0
        ).astype(jnp.bfloat16)
        scaled = jnp.dot(picks[:, :tok_count], grads[r], preferred_element_type=jnp.float32)
        for e in range(EXPERTS):
            packed[r, e] = scaled[e * CAP : (e + 1) * CAP].astype(jnp.bfloat16)

    for copy in near:
        copy.start()
    exchanges[1].start()
    start_hop(0, 1)
    for copy in exchanges[2:]:
        copy.start()
    for copy in own:
        copy.start()
    spread = []
    for i in range(1, ep_count + last_hop):
        if i < ep_count:
            exchanges[i].wait_recv()
            start_hop(i, 1)
        if i == 1:
            for copy in near:
                copy.wait()
            for copy in own:
                copy.wait()
            for r in range(rep_count):
                pack(r)
        for distance in range(1, last_hop + 1):
            j = i - distance
            if 0 <= j < ep_count:
                for way in (1, -1):
                    hops[j, way, distance].wait_recv()
                start_hop(j, distance + 1)
        if i == ep_count // 2 + 1:
            spread.append(
                pltpu.make_async_copy(packed.at[:, ep // group], cols_ref.at[:, ep], own_sem.at[3])
            )
            for k in range(1, ep_count):
                dest = steps[k][0](ep)
                spread.append(
                    remote(
                        packed.at[:, dest // group], cols_ref.at[:, ep],
                        cols_send.at[k], cols_recv.at[k], rep, dest,
                    )
                )
            for copy in spread:
                copy.start()
    for copy in spread:
        copy.wait()
    for copy in exchanges[1:]:
        copy.wait_send()
    for copy in hops.values():
        copy.wait_send()


def exchange(hidden, grad, route, rep_count, ep_count):
    unit_cols = hidden.shape[2] * EXPERTS // ep_count
    tok_count = grad.shape[0]
    col_width = grad.shape[1] // rep_count
    hops = max(1, rep_count // 2)
    dma = pltpu.SemaphoreType.DMA
    return pl.pallas_call(
        functools.partial(exchange_kernel, rep_count, ep_count),
        out_shape=(
            jax.ShapeDtypeStruct((rep_count, ep_count, CAP, unit_cols), jnp.bfloat16),
            jax.ShapeDtypeStruct((rep_count, ep_count, CAP, col_width), jnp.bfloat16),
        ),
        in_specs=[
            pl.BlockSpec(memory_space=pl.ANY),
            pl.BlockSpec(memory_space=pltpu.HBM),
            pl.BlockSpec(memory_space=pl.ANY),
        ],
        out_specs=(pl.BlockSpec(memory_space=pl.ANY),) * 2,
        scratch_shapes=[
            pltpu.VMEM((rep_count, tok_count, col_width), jnp.bfloat16),
            pltpu.VMEM((rep_count,) + route.shape, jnp.bfloat16),
            pltpu.VMEM((rep_count, EXPERTS, CAP, col_width), jnp.bfloat16),
            dma((4,)),
            dma((ep_count,)),
            dma((ep_count,)),
            dma((2, hops, ep_count)),
            dma((2, hops, ep_count)),
            dma((rep_count,)),
            dma((rep_count,)),
            dma((rep_count,)),
            dma((rep_count,)),
            dma((ep_count,)),
            dma((ep_count,)),
        ],
        compiler_params=pltpu.CompilerParams(
            has_side_effects=True, vmem_limit_bytes=4 * 1024 * 1024
        ),
    )(hidden, grad, route)


def per_device(out_grad, saved_hidden, combine, expert_ids):
    ep_count = lax.axis_size("ep")
    rep_count = lax.axis_size("rep")
    tok_count, model_width = out_grad.shape
    units = saved_hidden.shape[2]
    lanes = -(-tok_count // 128) * 128
    small = lax.optimization_barrier(
        jnp.concatenate([expert_ids.T.astype(jnp.float32), combine.T.astype(jnp.float32)], axis=0)
    )
    ids, probs = small[:TOP], small[TOP:]
    experts = jnp.arange(EXPERTS, dtype=jnp.int32).astype(jnp.float32)
    chosen = ids[:, None, :] == experts[None, :, None]
    named = jnp.any(chosen, axis=0)
    weight = jnp.sum(jnp.where(chosen, probs[:, None, :], jnp.float32(0.0)), axis=0)
    route = jnp.concatenate([weight, named.astype(jnp.float32)], axis=0).astype(jnp.bfloat16)
    route = jnp.pad(route, ((0, 0), (0, lanes - tok_count)))
    before = jnp.arange(tok_count)[:, None] < jnp.arange(tok_count)[None, :]
    row = jnp.dot(
        named.astype(jnp.bfloat16), before.astype(jnp.bfloat16), preferred_element_type=jnp.float32
    )
    slots = jnp.arange(CAP, dtype=jnp.float32)
    at_slot = row[:, None, None, :] == slots[None, :, None, None]
    pick = (at_slot & chosen.transpose(1, 0, 2)[:, None]).astype(jnp.bfloat16)
    send_hidden = lax.dot_general(
        pick.reshape(EXPERTS * CAP, TOP, tok_count),
        saved_hidden,
        (((1, 2), (1, 0)), ((), ())),
        preferred_element_type=jnp.float32,
    ).astype(jnp.bfloat16)
    rows, cols = exchange(
        send_hidden.reshape(EXPERTS, CAP, units), out_grad, route, rep_count, ep_count
    )
    row_total = rep_count * ep_count * CAP
    return lax.dot_general(
        rows.reshape(row_total, rows.shape[3]),
        cols.reshape(row_total, cols.shape[3]),
        (((0,), (0,)), ((), ())),
        preferred_element_type=jnp.float32,
    )


def solution(mesh):
    in_specs = (
        P(("rep", "ep"), None),
        P(("rep", "ep"), None, None),
        P(("rep", "ep"), None),
        P(("rep", "ep"), None),
    )
    out_specs = P("ep", "rep")
    return jax.shard_map(
        per_device, mesh=mesh, in_specs=in_specs, out_specs=out_specs, check_vma=False
    )
```
